32 devices in a mesh: data: 1 (over z), time: 32 (over y, x, core).
Axes of the slice: x: 4, y: 4, z: 1, core: 2. Of those that a mesh axis runs over, the one named last changes fastest.
The devices are a block of a 4x4x8 slice.
Arguments:
- x_init: float32 [16, 256, 16], P('data')
- w_in: bfloat16 [16, 768], replicated
- w_out: bfloat16 [768, 16], replicated
- mod_scale: bfloat16 [64, 768], P('time')
- mod_shift: bfloat16 [64, 768], P('time')
- step_size: float32 [64], P('time')
- noise_inc: float32 [64, 16, 256, 16], P('time', 'data')
Outputs:
- output: float32 [64, 16, 256, 16], P('time', 'data')
All inputs are finite; a program needn't handle non-finite values.
Results may differ from the reference program's by a relative error of at most 0.001.
Values are sent between devices in bfloat16 or wider.
A program may use at most 768 MiB of HBM per device.

```python
import jax
import jax.numpy as jnp
from jax import lax

BATCH = 16
TOKENS = 256
CHANNELS = 16
HIDDEN = 768
STEPS = 64
SWEEPS = 8


def setup_inputs(seed: int = 0, part: int = 0) -> dict:
    base_key = jax.random.key(seed)
    part_key = jax.random.fold_in(base_key, part)
    key_lat, key_noise = jax.random.split(part_key, 2)
    key_list = jax.random.split(jax.random.key(seed + 1), 6)
    w_first = jax.random.normal(key_list[0], (CHANNELS, HIDDEN), jnp.float32) * CHANNELS ** -0.5
    w_back = -(2.0 * CHANNELS / HIDDEN) * w_first.T + 0.5 * HIDDEN ** -0.5 * jax.random.normal(key_list[1], (HIDDEN, CHANNELS), jnp.float32)
    mod_scale = 0.2 * jax.random.normal(key_list[2], (STEPS, HIDDEN), jnp.float32)
    mod_shift = 0.5 * jax.random.normal(key_list[3], (STEPS, HIDDEN), jnp.float32)
    position = (jnp.arange(STEPS, dtype=jnp.float32) + 0.5) / STEPS
    tilt_coef = jax.random.uniform(key_list[4], (), jnp.float32, -1.0, 1.0)
    jitter = jax.random.uniform(key_list[5], (STEPS,), jnp.float32, 0.75, 1.25)
    step_size = (3.0 / STEPS) * jnp.exp(tilt_coef * (position - 0.5)) * jitter
    x_init = jax.random.normal(key_lat, (BATCH, TOKENS, CHANNELS), jnp.float32)
    noise_inc = 2.0 * STEPS ** -0.5 * jax.random.normal(key_noise, (STEPS, BATCH, TOKENS, CHANNELS), jnp.float32)
    return {
        "x_init": x_init,
        "w_in": w_first.astype(jnp.bfloat16),
        "w_out": w_back.astype(jnp.bfloat16),
        "mod_scale": mod_scale.astype(jnp.bfloat16),
        "mod_shift": mod_shift.astype(jnp.bfloat16),
        "step_size": step_size,
        "noise_inc": noise_inc,
    }


def drift_one(latents, scale_row, shift_row, step_row, w_in, w_out):
    flat_lat = latents.astype(jnp.bfloat16).reshape(BATCH * TOKENS, CHANNELS)
    pre_act = jnp.dot(flat_lat, w_in, preferred_element_type=jnp.float32)
    hidden = pre_act * (1.0 + scale_row.astype(jnp.float32)) + shift_row.astype(jnp.float32)
    gelu_out = jax.nn.gelu(hidden, approximate=True).astype(jnp.bfloat16)
    proj_out = jnp.dot(gelu_out, w_out, preferred_element_type=jnp.float32)
    return (step_row * proj_out).reshape(BATCH, TOKENS, CHANNELS)


def reference(x_init, w_in, w_out, mod_scale, mod_shift, step_size, noise_inc):
    def one_sweep(latents, unused):
        drifts = lax.map(lambda fields: drift_one(fields[0], fields[1], fields[2], fields[3], w_in, w_out), (latents, mod_scale, mod_shift, step_size))
        increments = drifts + noise_inc
        earlier = jnp.concatenate([jnp.zeros_like(increments[:1]), jnp.cumsum(increments[:-1], axis=0)], axis=0)
        return x_init[None] + earlier, None
    start_lat = jnp.broadcast_to(x_init[None], noise_inc.shape)
    final_lat, unused = lax.scan(one_sweep, start_lat, None, length=SWEEPS)
    return final_lat
```

```python
import functools
import math

import jax
import jax.numpy as jnp
from jax import lax
from jax.experimental import pallas as pl
from jax.experimental.pallas import tpu as pltpu
from jax.sharding import PartitionSpec as P

SWEEPS = 8
UNROLL = 16
SLOTS = 4
LIN = 2.0 * math.sqrt(2.0 / math.pi)
CUB = 8.0 * 0.044715 * math.sqrt(2.0 / math.pi)
F32, BF16 = jnp.float32, jnp.bfloat16


def kernel(n, own, x0_hbm, w_in, w_out, scale, shift, step, noise_hbm, out_hbm, weights, rhs, gathered, turned, base_tab,
           scale_all, shift_all, step_all, noise_all, x_all, x0, run, staged, *rest):
    hid, act = rest[:SLOTS], rest[SLOTS:2 * SLOTS]
    send_mod, recv_mod, send_noise, recv_noise, send_out, recv_out, local_sem = rest[2 * SLOTS:]
    me = lax.axis_index("time")
    chan, hidden = w_in.shape
    tok = x0.shape[1]
    per_row = x0_hbm.shape[2] // tok

    def chunk(dev):
        return dev // per_row, pl.ds(pl.multiple_of((dev % per_row) * tok, tok), tok)

    my_row, my_cols = chunk(me)

    def peer(k):
        return lax.rem(me + k, n)

    barrier = pltpu.get_barrier_semaphore()

    @pl.loop(1, n)
    def _(k):
        pl.semaphore_signal(barrier, inc=1, device_id={"time": peer(k)}, device_id_type=pl.DeviceIdType.MESH)

    first = pltpu.make_async_copy(x0_hbm.at[my_row, :, my_cols], x0, local_sem.at[0])
    first.start()
    mine = pltpu.make_async_copy(noise_hbm.at[:, my_row, :, my_cols], noise_all.at[me], local_sem.at[1])
    mine.start()
    scale_all[me] = scale[...]
    shift_all[me] = shift[...]
    for s in range(own):
        step_all[me, s:s + 1, :] = jnp.full((1, tok), step[s], F32)
    gathered[...] = jnp.zeros_like(gathered)
    first.wait()
    mine.wait()
    pl.semaphore_wait(barrier, n - 1)

    def mod_copies(dst, src_dev, k):
        pairs = ((scale, scale_all), (shift, shift_all), (step_all.at[me], step_all))
        return [
            pltpu.make_async_remote_copy(src_ref=a, dst_ref=b.at[src_dev], send_sem=send_mod.at[i, k], recv_sem=recv_mod.at[i, src_dev],
                                         device_id={"time": dst}, device_id_type=pl.DeviceIdType.MESH)
            for i, (a, b) in enumerate(pairs)
        ]

    def noise_copy(dst, src_dev, k):
        row, cols = chunk(dst)
        return pltpu.make_async_remote_copy(src_ref=noise_hbm.at[:, row, :, cols], dst_ref=noise_all.at[src_dev], send_sem=send_noise.at[k],
                                            recv_sem=recv_noise.at[src_dev], device_id={"time": dst}, device_id_type=pl.DeviceIdType.MESH)

    def out_copy(dst, src_dev, k):
        row, cols = chunk(src_dev)
        return pltpu.make_async_remote_copy(src_ref=x_all.at[dst], dst_ref=out_hbm.at[:, row, :, cols], send_sem=send_out.at[k],
                                            recv_sem=recv_out.at[src_dev], device_id={"time": dst}, device_id_type=pl.DeviceIdType.MESH)

    @pl.loop(1, n)
    def _(k):
        for copy in mod_copies(peer(k), me, k):
            copy.start()

    @pl.loop(1, n)
    def _(k):
        noise_copy(peer(k), me, k).start()

    x_first = x0[...]
    xb = x_first.astype(BF16)
    block = jnp.concatenate([xb, xb, xb, jnp.ones_like(xb)], axis=0)
    nothing = jnp.zeros_like(block)
    both = jnp.concatenate([jnp.concatenate([block, nothing], axis=1), jnp.concatenate([nothing, block], axis=1)], axis=0)

    @pl.loop(0, n)
    def _(q):
        rhs[q] = both

    run[...] = x_first
    for u in range(UNROLL):
        for t in range(own):
            staged[u, t] = xb

    @pl.loop(1, n)
    def _(k):
        source = lax.rem(me - k + n, n)
        for copy in mod_copies(peer(k), source, k):
            copy.wait_recv()

    rows = 2 * own * n
    for p in range(n):
        gathered[2 * own * p:2 * own * p + own, :] = scale_all[p].astype(F32)
        gathered[2 * own * p + own:2 * own * (p + 1), :] = shift_all[p].astype(F32)
    gathered[rows:rows + chan, :] = w_in[...].astype(F32)
    gathered[rows + chan:rows + chan + 8, :] = jnp.ones((8, hidden), F32)
    turned[...] = jnp.transpose(gathered[...]).astype(BF16)

    width = 64
    depth = gathered.shape[0]
    k_id = lax.broadcasted_iota(jnp.int32, (depth, 2 * width), 0)
    lane = lax.broadcasted_iota(jnp.int32, (depth, 2 * width), 1)
    part = lane % width
    which = lane // width
    pick_w = (part < 3 * chan) & (k_id == rows + part % chan)
    lane_row = lax.broadcasted_iota(jnp.int32, (1, 2 * width), 1) % width
    base_tab[...] = 0.5 * jnp.dot(turned[...], jnp.where(pick_w, 1.0, 0.0).astype(BF16), preferred_element_type=F32) + jnp.where(
        lane_row == 3 * chan, 0.5, 0.0)
    low_mask = jnp.where((lane_row >= 2 * chan) & (lane_row < 3 * chan), 1.0, 0.0)
    target = jnp.where(part < chan, rows + chan, jnp.where(part < 3 * chan, which, jnp.where(part == 3 * chan, own + which, depth)))
    moving = jnp.where((part >= chan) & (part <= 3 * chan), 2 * own, 0)

    @pl.loop(0, n // 2)
    def _(q2):
        picks = [jnp.where(k_id == target + moving * (2 * q2 + j), 1.0, 0.0).astype(BF16) for j in range(2)]
        factor = jnp.dot(turned[...], jnp.concatenate(picks, axis=1), preferred_element_type=F32)
        for j in range(2):
            value = base_tab[...] * factor[:, 2 * width * j:2 * width * (j + 1)]
            high = value.astype(BF16).astype(F32)
            weights[2 * q2 + j] = (value - high * low_mask).astype(BF16)

    @pl.loop(1, n)
    def _(k):
        source = lax.rem(me - k + n, n)
        noise_copy(peer(k), source, k).wait_recv()

    def first_product(q, slot):
        hid[slot][...] = jnp.dot(weights[q], rhs[q], preferred_element_type=F32)

    def activate(slot):
        g = hid[slot][...]
        act[slot][...] = g * (1.0 + jnp.tanh(g * (LIN + CUB * (g * g))))

    def second_product(q, slot, u):
        drift = jnp.dot(w_out[...].astype(F32), act[slot][...], preferred_element_type=F32)
        x = jnp.where(q == 0, x0[...], run[...])
        for t in range(own):
            x_all[q, t] = x
            if u is not None:
                staged[u, t] = x.astype(BF16)
            x = x + (drift[:, tok * t:tok * (t + 1)] * step_all[q, t:t + 1, :] + noise_all[q, t])
        run[...] = x

    first_product(0, 0)
    first_product(1, 1)

    def trip(i, carry):
        base = i * UNROLL
        for u in range(UNROLL):
            q = lax.rem(base + 2 * n - 1 - UNROLL + u, n)
            for t in range(own):
                xb = staged[u, t]
                for j in range(3):
                    rhs[q, width * t + chan * j:width * t + chan * (j + 1), tok * t:tok * (t + 1)] = xb
        for u in range(UNROLL):
            second_product(lax.rem(base + n - 1 + u, n), (u - 1) % SLOTS, u)
            activate(u % SLOTS)
            first_product(lax.rem(base + u + 2, n), (u + 2) % SLOTS)
        return carry

    lax.fori_loop(0, SWEEPS * n // UNROLL, trip, 0)
    second_product(n - 1, (UNROLL - 1) % SLOTS, None)

    @pl.loop(1, n)
    def _(k):
        out_copy(peer(k), me, k).start()

    last = pltpu.make_async_copy(x_all.at[me], out_hbm.at[:, my_row, :, my_cols], local_sem.at[0])
    last.start()
    last.wait()

    @pl.loop(1, n)
    def _(k):
        source = lax.rem(me - k + n, n)
        out_copy(peer(k), source, k).wait_recv()

    @pl.loop(1, n)
    def _(k):
        for copy in mod_copies(peer(k), me, k):
            copy.wait_send()
        noise_copy(peer(k), me, k).wait_send()
        out_copy(peer(k), me, k).wait_send()


def solution(mesh):
    n = mesh.shape["time"]

    def body(x_init, w_in, w_out, mod_scale, mod_shift, step_size, noise_inc):
        own, batch, tokens, chan = noise_inc.shape
        hidden = w_in.shape[1]
        tok = batch * tokens // n
        vmem, hbm, smem = (pl.BlockSpec(memory_space=m) for m in (pltpu.VMEM, pl.ANY, pltpu.SMEM))
        out = pl.pallas_call(
            functools.partial(kernel, n, own),
            out_shape=jax.ShapeDtypeStruct((own, batch, chan, tokens), F32),
            in_specs=[hbm, vmem, vmem, vmem, vmem, smem, hbm],
            out_specs=hbm,
            scratch_shapes=[
                pltpu.VMEM((n, hidden, 128), BF16),
                pltpu.VMEM((n, 128, own * tok), BF16),
                pltpu.VMEM((256, hidden), F32),
                pltpu.VMEM((hidden, 256), BF16),
                pltpu.VMEM((hidden, 128), F32),
                pltpu.VMEM((n, own, hidden), BF16),
                pltpu.VMEM((n, own, hidden), BF16),
                pltpu.VMEM((n, own, tok), F32),
                pltpu.VMEM((n, own, chan, tok), F32),
                pltpu.VMEM((n, own, chan, tok), F32),
                pltpu.VMEM((chan, tok), F32),
                pltpu.VMEM((chan, tok), F32),
                pltpu.VMEM((UNROLL, own, chan, tok), BF16),
            ]
            + [pltpu.VMEM((hidden, own * tok), F32)] * SLOTS
            + [pltpu.VMEM((hidden, own * tok), F32)] * SLOTS
            + [
                pltpu.SemaphoreType.DMA((3, n)),
                pltpu.SemaphoreType.DMA((3, n)),
                pltpu.SemaphoreType.DMA((n,)),
                pltpu.SemaphoreType.DMA((n,)),
                pltpu.SemaphoreType.DMA((n,)),
                pltpu.SemaphoreType.DMA((n,)),
                pltpu.SemaphoreType.DMA((2,)),
            ],
            compiler_params=pltpu.CompilerParams(collective_id=0, has_side_effects=True, vmem_limit_bytes=56 * 1024 * 1024),
            name="picard",
        )(jnp.swapaxes(x_init, 1, 2), w_in, w_out.T, mod_scale, mod_shift, step_size, jnp.swapaxes(noise_inc, 2, 3))
        return jnp.swapaxes(out, 2, 3)

    return jax.shard_map(
        body,
        mesh=mesh,
        in_specs=(P("data"), P(), P(), P("time"), P("time"), P("time"), P("time", "data")),
        out_specs=P("time", "data"),
        check_vma=False,
    )
```

```python
import functools
import math

import jax
import jax.numpy as jnp
from jax import lax
from jax.experimental import pallas as pl
from jax.experimental.pallas import tpu as pltpu
from jax.sharding import PartitionSpec as P

SWEEPS = 8
UNROLL = 16
SLOTS = 2
LIN = 2.0 * math.sqrt(2.0 / math.pi)
CUB = 8.0 * 0.044715 * math.sqrt(2.0 / math.pi)
F32, BF16 = jnp.float32, jnp.bfloat16


def kernel(n, own, x0_hbm, w_in, w_out, scale, shift, step, noise_hbm, out_hbm, weights, rhs, scale_all, shift_all, step_all, noise_all,
           drift_mine, x_all, x0, run, staged, *rest):
    hid, act = rest[:SLOTS], rest[SLOTS:2 * SLOTS]
    (send_scale, recv_scale, send_shift, recv_shift, send_step, recv_step, send_noise, recv_noise, send_out, recv_out, local_sem) = rest[2 * SLOTS:]
    me = lax.axis_index("time")
    chan, hidden = w_in.shape
    tok = x0.shape[1]
    width = 64
    per_row = x0_hbm.shape[2] // tok

    def chunk(dev):
        return dev // per_row, pl.ds(pl.multiple_of((dev % per_row) * tok, tok), tok)

    my_row, my_cols = chunk(me)

    def peer(k):
        return lax.rem(me + k, n)

    def source(k):
        return lax.rem(me - k + n, n)

    def remote(src, dst, send_sem, recv_sem, dev):
        return pltpu.make_async_remote_copy(src_ref=src, dst_ref=dst, send_sem=send_sem, recv_sem=recv_sem, device_id={"time": dev},
                                            device_id_type=pl.DeviceIdType.MESH)

    def scale_copy(dst, src_dev, k):
        return remote(scale, scale_all.at[src_dev], send_scale.at[k], recv_scale.at[src_dev], dst)

    def shift_copy(dst, src_dev, k):
        return remote(shift, shift_all.at[src_dev], send_shift.at[k], recv_shift.at[src_dev], dst)

    def step_copy(dst, src_dev, k):
        return remote(step_all.at[me], step_all.at[src_dev], send_step.at[k], recv_step.at[src_dev], dst)

    def noise_copy(dst, src_dev, k):
        row, cols = chunk(dst)
        return remote(noise_hbm.at[:, row, :, cols], noise_all.at[src_dev], send_noise.at[k], recv_noise.at[src_dev], dst)

    def out_copy(dst, src_dev, k):
        row, cols = chunk(src_dev)
        return remote(x_all.at[dst], out_hbm.at[:, row, :, cols], send_out.at[k], recv_out.at[src_dev], dst)

    barrier = pltpu.get_barrier_semaphore()

    @pl.loop(1, n)
    def _(k):
        pl.semaphore_signal(barrier, inc=1, device_id={"time": peer(k)}, device_id_type=pl.DeviceIdType.MESH)

    local = [
        pltpu.make_async_copy(x0_hbm.at[my_row, :, my_cols], x0, local_sem.at[0]),
        pltpu.make_async_copy(noise_hbm.at[:, my_row, :, my_cols], noise_all.at[me], local_sem.at[1]),
    ]
    for copy in local:
        copy.start()
    scale_all[me] = scale[...]
    shift_all[me] = shift[...]
    for t in range(own):
        step_all[me, t:t + 1, :] = jnp.full((1, tok), step[t], F32)

    half = 0.5 * w_in[...].astype(F32)
    top = lax.broadcasted_iota(jnp.int32, (chan, hidden), 0) == 0

    def modulated(scales, shifts):
        scales, shifts = scales.astype(F32), shifts.astype(F32)
        parts = []
        for t in range(own):
            value = half * scales[t:t + 1, :]
            high = value.astype(BF16)
            low = (value - high.astype(F32)).astype(BF16)
            bias = jnp.where(top, 0.5 * shifts[t:t + 1, :], 0.0).astype(BF16)
            parts += [half.astype(BF16), high, low, bias]
        return jnp.transpose(jnp.concatenate(parts, axis=0))

    for copy in local:
        copy.wait()

    xb = x0[...].astype(BF16)
    block = jnp.concatenate([xb, xb, xb, jnp.ones_like(xb)], axis=0)
    nothing = jnp.zeros_like(block)
    both = jnp.concatenate([jnp.concatenate([block, nothing], axis=1), jnp.concatenate([nothing, block], axis=1)], axis=0)

    @pl.loop(0, n)
    def _(q):
        rhs[q] = both

    def put_latents(q, t, xb):
        for j in range(3):
            rhs[q, width * t + chan * j:width * t + chan * (j + 1), tok * t:tok * (t + 1)] = xb

    def first_product(w, q, slot):
        right = rhs[q]
        for part in range(2):
            rows = slice(part * hidden // 2, (part + 1) * hidden // 2)
            hid[slot][rows, :] = jnp.dot(weights[w, rows, :], right, preferred_element_type=F32)

    def activate(slot):
        g = hid[slot][...]
        act[slot][...] = g * (1.0 + jnp.tanh(g * (LIN + CUB * (g * g))))

    def second_product(slot):
        return jnp.dot(w_out[...].astype(F32), act[slot][...], preferred_element_type=F32)

    def sweep(into):
        def finish(q, slot):
            drift = second_product(slot)
            for t in range(own):
                into[q, t] = drift[:, tok * t:tok * (t + 1)] * step_all[q, t:t + 1, :]

        weights[0] = modulated(scale_all[0], shift_all[0])
        first_product(0, 0, 0)

        def trip(i, carry):
            base = i * UNROLL
            for u in range(UNROLL):
                nxt = lax.rem(base + u + 1, n)
                weights[nxt] = modulated(scale_all[nxt], shift_all[nxt])
                finish(lax.rem(base + n - 1 + u, n), (u - 1) % SLOTS)
                activate(u % SLOTS)
                first_product(nxt, nxt, (u + 1) % SLOTS)
            return carry

        lax.fori_loop(0, n // UNROLL, trip, 0)
        finish(n - 1, (UNROLL - 1) % SLOTS)

    pl.semaphore_wait(barrier, n - 1)

    @pl.loop(1, n)
    def _(k):
        scale_copy(peer(k), me, k).start()
        shift_copy(peer(k), me, k).start()
        step_copy(peer(k), me, k).start()

    @pl.loop(1, n)
    def _(k):
        noise_copy(peer(k), me, k).start()

    @pl.loop(1, n)
    def _(k):
        scale_copy(peer(k), source(k), k).wait_recv()
        shift_copy(peer(k), source(k), k).wait_recv()

    @pl.loop(1, n)
    def _(k):
        step_copy(peer(k), source(k), k).wait_recv()

    sweep(drift_mine)

    @pl.loop(1, n)
    def _(k):
        noise_copy(peer(k), source(k), k).wait_recv()

    x = x0[...]
    for q in range(n):
        for t in range(own):
            xb = x.astype(BF16)
            put_latents(q, t, xb)
            if q >= n - 1 - UNROLL and q < n - 1:
                staged[q - (n - 1 - UNROLL), t] = xb
            if q == n - 1 and t == 0:
                run[...] = x
            x = x + (drift_mine[q, t] + noise_all[q, t])

    def advance(q, slot, u):
        change = second_product(slot)
        x = jnp.where(q == 0, x0[...], run[...])
        for t in range(own):
            x_all[q, t] = x
            if u is not None:
                staged[u, t] = x.astype(BF16)
            x = x + (change[:, tok * t:tok * (t + 1)] * step_all[q, t:t + 1, :] + noise_all[q, t])
        run[...] = x

    first_product(0, 0, 0)

    def trip(i, carry):
        base = i * UNROLL
        for u in range(UNROLL):
            late = lax.rem(base + 2 * n - 1 - UNROLL + u, n)
            for t in range(own):
                put_latents(late, t, staged[u, t])
            advance(lax.rem(base + n - 1 + u, n), (u - 1) % SLOTS, u)
            activate(u % SLOTS)
            q = lax.rem(base + u + 1, n)
            first_product(q, q, (u + 1) % SLOTS)
        return carry

    trips = (SWEEPS - 1) * n // UNROLL
    early = n - UNROLL - 1
    lax.fori_loop(0, trips - 1, trip, 0)

    def deliver(first_dev, count):
        @pl.loop(0, count)
        def _(k):
            dst = first_dev + lax.rem(me + k, count)

            @pl.when(dst != me)
            def _():
                out_copy(dst, me, lax.rem(dst - me + n, n)).start()

    deliver(0, early)
    trip(trips - 1, 0)
    advance(n - 1, (UNROLL - 1) % SLOTS, None)
    deliver(early, n - early)

    last = pltpu.make_async_copy(x_all.at[me], out_hbm.at[:, my_row, :, my_cols], local_sem.at[0])
    last.start()
    last.wait()

    @pl.loop(1, n)
    def _(k):
        out_copy(peer(k), source(k), k).wait_recv()

    @pl.loop(1, n)
    def _(k):
        scale_copy(peer(k), me, k).wait_send()
        shift_copy(peer(k), me, k).wait_send()
        step_copy(peer(k), me, k).wait_send()
        noise_copy(peer(k), me, k).wait_send()
        out_copy(peer(k), me, k).wait_send()


def solution(mesh):
    n = mesh.shape["time"]

    def body(x_init, w_in, w_out, mod_scale, mod_shift, step_size, noise_inc):
        own, batch, tokens, chan = noise_inc.shape
        hidden = w_in.shape[1]
        tok = batch * tokens // n
        vmem, hbm, smem = (pl.BlockSpec(memory_space=m) for m in (pltpu.VMEM, pl.ANY, pltpu.SMEM))
        out = pl.pallas_call(
            functools.partial(kernel, n, own),
            out_shape=jax.ShapeDtypeStruct((own, batch, chan, tokens), F32),
            in_specs=[hbm, vmem, vmem, vmem, vmem, smem, hbm],
            out_specs=hbm,
            scratch_shapes=[
                pltpu.VMEM((n, hidden, 128), BF16),
                pltpu.VMEM((n, 128, own * tok), BF16),
                pltpu.VMEM((n, own, hidden), BF16),
                pltpu.VMEM((n, own, hidden), BF16),
                pltpu.VMEM((n, own, tok), F32),
            ]
            + [pltpu.VMEM((n, own, chan, tok), F32)] * 3
            + [
                pltpu.VMEM((chan, tok), F32),
                pltpu.VMEM((chan, tok), F32),
                pltpu.VMEM((UNROLL, own, chan, tok), BF16),
            ]
            + [pltpu.VMEM((hidden, own * tok), F32)] * (2 * SLOTS)
            + [pltpu.SemaphoreType.DMA((n,))] * 10
            + [pltpu.SemaphoreType.DMA((2,))],
            compiler_params=pltpu.CompilerParams(collective_id=0, has_side_effects=True, vmem_limit_bytes=40 * 1024 * 1024),
            name="picard",
        )(jnp.swapaxes(x_init, 1, 2), w_in, w_out.T, mod_scale, mod_shift, step_size, jnp.swapaxes(noise_inc, 2, 3))
        return jnp.swapaxes(out, 2, 3)

    return jax.shard_map(
        body,
        mesh=mesh,
        in_specs=(P("data"), P(), P(), P("time"), P("time"), P("time"), P("time", "data")),
        out_specs=P("time", "data"),
        check_vma=False,
    )
```

```python
import functools
import math

import jax
import jax.numpy as jnp
from jax import lax
from jax.experimental import pallas as pl
from jax.experimental.pallas import tpu as pltpu
from jax.sharding import PartitionSpec as P

SWEEPS = 8
FIRST_UNROLL = 16
UNROLL = 18
SLOTS = 2
LIN = 2.0 * math.sqrt(2.0 / math.pi)
CUB = 8.0 * 0.044715 * math.sqrt(2.0 / math.pi)
F32, BF16 = jnp.float32, jnp.bfloat16


def plan(n, own):
    starts = [(k - 1) // own for k in range(2, SWEEPS + 1)]
    spare = -sum(n - first for first in starts) % UNROLL
    for i in range(len(starts)):
        back = min(spare, starts[i], 1)
        if starts[i] > 1 or spare > sum(1 for later in starts[i + 1:] if later > 1):
            starts[i] -= back
            spare -= back
    ends, total = [], 0
    for first in starts:
        total += n - first
        ends.append(total)
    assert spare == 0 and total % UNROLL == 0
    return starts, ends


def kernel(n, own, x0_hbm, w_in, w_out, scale, shift, step, noise_hbm, out_hbm, weights, rhs, scale_all, shift_all, step_all, noise_all,
           drift_mine, x_all, x0, run, staged, *rest):
    hid, act = rest[:SLOTS], rest[SLOTS:2 * SLOTS]
    (send_scale, recv_scale, send_shift, recv_shift, send_step, recv_step, send_noise, recv_noise, send_out, recv_out, local_sem) = rest[2 * SLOTS:]
    me = lax.axis_index("time")
    chan, hidden = w_in.shape
    tok = x0.shape[1]
    width = 64
    per_row = x0_hbm.shape[2] // tok

    def chunk(dev):
        return dev // per_row, pl.ds(pl.multiple_of((dev % per_row) * tok, tok), tok)

    my_row, my_cols = chunk(me)

    def peer(k):
        return lax.rem(me + k, n)

    def source(k):
        return lax.rem(me - k + n, n)

    def remote(src, dst, send_sem, recv_sem, dev):
        return pltpu.make_async_remote_copy(src_ref=src, dst_ref=dst, send_sem=send_sem, recv_sem=recv_sem, device_id={"time": dev},
                                            device_id_type=pl.DeviceIdType.MESH)

    def scale_copy(dst, src_dev, k):
        return remote(scale, scale_all.at[src_dev], send_scale.at[k], recv_scale.at[src_dev], dst)

    def shift_copy(dst, src_dev, k):
        return remote(shift, shift_all.at[src_dev], send_shift.at[k], recv_shift.at[src_dev], dst)

    def step_copy(dst, src_dev, k):
        return remote(step_all.at[me], step_all.at[src_dev], send_step.at[k], recv_step.at[src_dev], dst)

    def noise_copy(dst, src_dev, k):
        row, cols = chunk(dst)
        return remote(noise_hbm.at[:, row, :, cols], noise_all.at[src_dev], send_noise.at[k], recv_noise.at[src_dev], dst)

    def out_copy(dst, src_dev, k):
        row, cols = chunk(src_dev)
        return remote(x_all.at[dst], out_hbm.at[:, row, :, cols], send_out.at[k], recv_out.at[src_dev], dst)

    barrier = pltpu.get_barrier_semaphore()

    @pl.loop(1, n)
    def _(k):
        pl.semaphore_signal(barrier, inc=1, device_id={"time": peer(k)}, device_id_type=pl.DeviceIdType.MESH)

    local = [
        pltpu.make_async_copy(x0_hbm.at[my_row, :, my_cols], x0, local_sem.at[0]),
        pltpu.make_async_copy(noise_hbm.at[:, my_row, :, my_cols], noise_all.at[me], local_sem.at[1]),
    ]
    for copy in local:
        copy.start()
    scale_all[me] = scale[...]
    shift_all[me] = shift[...]
    for t in range(own):
        step_all[me, t:t + 1, :] = jnp.full((1, tok), step[t], F32)

    half = 0.5 * w_in[...].astype(F32)
    top = lax.broadcasted_iota(jnp.int32, (chan, hidden), 0) == 0

    def modulated(scales, shifts):
        scales, shifts = scales.astype(F32), shifts.astype(F32)
        parts = []
        for t in range(own):
            value = half * scales[t:t + 1, :]
            high = value.astype(BF16)
            low = (value - high.astype(F32)).astype(BF16)
            bias = jnp.where(top, 0.5 * shifts[t:t + 1, :], 0.0).astype(BF16)
            parts += [half.astype(BF16), high, low, bias]
        return jnp.transpose(jnp.concatenate(parts, axis=0))

    for copy in local:
        copy.wait()

    xb = x0[...].astype(BF16)
    block = jnp.concatenate([xb, xb, xb, jnp.ones_like(xb)], axis=0)
    nothing = jnp.zeros_like(block)
    both = jnp.concatenate([jnp.concatenate([block, nothing], axis=1), jnp.concatenate([nothing, block], axis=1)], axis=0)

    @pl.loop(0, n)
    def _(q):
        rhs[q] = both

    def put_latents(q, t, xb):
        for j in range(3):
            rhs[q, width * t + chan * j:width * t + chan * (j + 1), tok * t:tok * (t + 1)] = xb

    def first_product(w, q, slot):
        right = rhs[q]
        for part in range(2):
            rows = slice(part * hidden // 2, (part + 1) * hidden // 2)
            hid[slot][rows, :] = jnp.dot(weights[w, rows, :], right, preferred_element_type=F32)

    def activate(slot):
        g = hid[slot][...]
        act[slot][...] = g * (1.0 + jnp.tanh(g * (LIN + CUB * (g * g))))

    def second_product(slot):
        return jnp.dot(w_out[...].astype(F32), act[slot][...], preferred_element_type=F32)

    def sweep(into):
        def finish(q, slot):
            drift = second_product(slot)
            for t in range(own):
                into[q, t] = drift[:, tok * t:tok * (t + 1)] * step_all[q, t:t + 1, :]

        weights[0] = modulated(scale_all[0], shift_all[0])
        first_product(0, 0, 0)

        def trip(i, carry):
            base = i * FIRST_UNROLL
            for u in range(FIRST_UNROLL):
                nxt = lax.rem(base + u + 1, n)
                weights[nxt] = modulated(scale_all[nxt], shift_all[nxt])
                finish(lax.rem(base + n - 1 + u, n), (u - 1) % SLOTS)
                activate(u % SLOTS)
                first_product(nxt, nxt, (u + 1) % SLOTS)
            return carry

        lax.fori_loop(0, n // FIRST_UNROLL, trip, 0)
        finish(n - 1, (FIRST_UNROLL - 1) % SLOTS)

    pl.semaphore_wait(barrier, n - 1)

    @pl.loop(1, n)
    def _(k):
        scale_copy(peer(k), me, k).start()
        shift_copy(peer(k), me, k).start()
        step_copy(peer(k), me, k).start()

    @pl.loop(1, n)
    def _(k):
        noise_copy(peer(k), me, k).start()

    @pl.loop(1, n)
    def _(k):
        scale_copy(peer(k), source(k), k).wait_recv()
        shift_copy(peer(k), source(k), k).wait_recv()

    @pl.loop(1, n)
    def _(k):
        step_copy(peer(k), source(k), k).wait_recv()

    sweep(drift_mine)

    @pl.loop(1, n)
    def _(k):
        noise_copy(peer(k), source(k), k).wait_recv()

    x = x0[...]
    for q in range(n):
        for t in range(own):
            xb = x.astype(BF16)
            put_latents(q, t, xb)
            if q >= n - 1 - UNROLL and q < n - 1:
                staged[q - (n - 1 - UNROLL), t] = xb
            if q == n - 1 and t == 0:
                run[...] = x
            x = x + (drift_mine[q, t] + noise_all[q, t])

    starts, ends = plan(n, own)

    def pair_of(p):
        q = p + jnp.where(p < 0, n, 0)
        for sweep_end, first in zip(ends[:-1], starts[1:]):
            q = q - jnp.where(p >= sweep_end, n - first, 0)
        return lax.rem(q, n)

    def advance(p, slot, u):
        q = pair_of(p)
        change = second_product(slot)
        opens = p == 0
        for sweep_end in ends[:-1]:
            opens = opens | (p == sweep_end)
        x = jnp.where(opens, x_all[q, 0], run[...])
        for t in range(own):
            x_all[q, t] = x
            if u is not None:
                staged[u, t] = x.astype(BF16)
            x = x + (change[:, tok * t:tok * (t + 1)] * step_all[q, t:t + 1, :] + noise_all[q, t])
        run[...] = x

    x_all[0, 0] = x0[...]
    first_product(0, 0, 0)

    def trip(i, carry):
        base = i * UNROLL
        for u in range(UNROLL):
            late = pair_of(base - 1 - UNROLL + u)
            for t in range(own):
                put_latents(late, t, staged[u, t])
            advance(base - 1 + u, (u - 1) % SLOTS, u)
            activate(u % SLOTS)
            q = pair_of(base + u + 1)
            first_product(q, q, (u + 1) % SLOTS)
        return carry

    trips = ends[-1] // UNROLL
    early = n - UNROLL - 1
    lax.fori_loop(0, trips - 1, trip, 0)

    def deliver(first_dev, count):
        @pl.loop(0, count)
        def _(k):
            dst = first_dev + lax.rem(me + k, count)

            @pl.when(dst != me)
            def _():
                out_copy(dst, me, lax.rem(dst - me + n, n)).start()

    deliver(0, early)
    trip(trips - 1, 0)
    advance(ends[-1] - 1, (UNROLL - 1) % SLOTS, None)
    deliver(early, n - early)

    last = pltpu.make_async_copy(x_all.at[me], out_hbm.at[:, my_row, :, my_cols], local_sem.at[0])
    last.start()
    last.wait()

    @pl.loop(1, n)
    def _(k):
        out_copy(peer(k), source(k), k).wait_recv()

    @pl.loop(1, n)
    def _(k):
        scale_copy(peer(k), me, k).wait_send()
        shift_copy(peer(k), me, k).wait_send()
        step_copy(peer(k), me, k).wait_send()
        noise_copy(peer(k), me, k).wait_send()
        out_copy(peer(k), me, k).wait_send()


def solution(mesh):
    n = mesh.shape["time"]

    def body(x_init, w_in, w_out, mod_scale, mod_shift, step_size, noise_inc):
        own, batch, tokens, chan = noise_inc.shape
        hidden = w_in.shape[1]
        tok = batch * tokens // n
        vmem, hbm, smem = (pl.BlockSpec(memory_space=m) for m in (pltpu.VMEM, pl.ANY, pltpu.SMEM))
        out = pl.pallas_call(
            functools.partial(kernel, n, own),
            out_shape=jax.ShapeDtypeStruct((own, batch, chan, tokens), F32),
            in_specs=[hbm, vmem, vmem, vmem, vmem, smem, hbm],
            out_specs=hbm,
            scratch_shapes=[
                pltpu.VMEM((n, hidden, 128), BF16),
                pltpu.VMEM((n, 128, own * tok), BF16),
                pltpu.VMEM((n, own, hidden), BF16),
                pltpu.VMEM((n, own, hidden), BF16),
                pltpu.VMEM((n, own, tok), F32),
            ]
            + [pltpu.VMEM((n, own, chan, tok), F32)] * 3
            + [
                pltpu.VMEM((chan, tok), F32),
                pltpu.VMEM((chan, tok), F32),
                pltpu.VMEM((UNROLL, own, chan, tok), BF16),
            ]
            + [pltpu.VMEM((hidden, own * tok), F32)] * (2 * SLOTS)
            + [pltpu.SemaphoreType.DMA((n,))] * 10
            + [pltpu.SemaphoreType.DMA((2,))],
            compiler_params=pltpu.CompilerParams(collective_id=0, has_side_effects=True, vmem_limit_bytes=40 * 1024 * 1024),
            name="picard",
        )(jnp.swapaxes(x_init, 1, 2), w_in, w_out.T, mod_scale, mod_shift, step_size, jnp.swapaxes(noise_inc, 2, 3))
        return jnp.swapaxes(out, 2, 3)

    return jax.shard_map(
        body,
        mesh=mesh,
        in_specs=(P("data"), P(), P(), P("time"), P("time"), P("time"), P("time", "data")),
        out_specs=P("time", "data"),
        check_vma=False,
    )
```

```python
import functools
import math

import jax
import jax.numpy as jnp
from jax import lax
from jax.experimental import pallas as pl
from jax.experimental.pallas import tpu as pltpu
from jax.sharding import PartitionSpec as P

SWEEPS = 8
FIRST_UNROLL = 16
UNROLL = 18
SLOTS = 2
LIN = 2.0 * math.sqrt(2.0 / math.pi)
CUB = 8.0 * 0.044715 * math.sqrt(2.0 / math.pi)
F32, BF16 = jnp.float32, jnp.bfloat16


def plan(n, own):
    starts = [(k - 1) // own for k in range(2, SWEEPS + 1)]
    spare = -sum(n - first for first in starts) % UNROLL
    for i in range(len(starts)):
        back = min(spare, starts[i], 1)
        if starts[i] > 1 or spare > sum(1 for later in starts[i + 1:] if later > 1):
            starts[i] -= back
            spare -= back
    ends, total = [], 0
    for first in starts:
        total += n - first
        ends.append(total)
    assert spare == 0 and total % UNROLL == 0
    return starts, ends


def kernel(n, own, x0_hbm, w_in, w_out, scale, shift, step, noise_hbm, out_hbm, weights, rhs, scale_all, shift_all, step_all, noise_all,
           drift_mine, x_all, x0, run, staged, *rest):
    hid, act = rest[:SLOTS], rest[SLOTS:2 * SLOTS]
    (send_scale, recv_scale, send_shift, recv_shift, send_step, recv_step, send_noise, recv_noise, send_out, recv_out, local_sem) = rest[2 * SLOTS:]
    me = lax.axis_index("time")
    chan, hidden = w_in.shape
    tok = x0.shape[1]
    width = 64
    per_row = x0_hbm.shape[2] // tok

    def chunk(dev):
        return dev // per_row, pl.ds(pl.multiple_of((dev % per_row) * tok, tok), tok)

    my_row, my_cols = chunk(me)

    def peer(k):
        return lax.rem(me + k, n)

    def source(k):
        return lax.rem(me - k + n, n)

    def remote(src, dst, send_sem, recv_sem, dev):
        return pltpu.make_async_remote_copy(src_ref=src, dst_ref=dst, send_sem=send_sem, recv_sem=recv_sem, device_id={"time": dev},
                                            device_id_type=pl.DeviceIdType.MESH)

    def scale_copy(dst, src_dev, k):
        return remote(scale, scale_all.at[src_dev], send_scale.at[k], recv_scale.at[src_dev], dst)

    def shift_copy(dst, src_dev, k):
        return remote(shift, shift_all.at[src_dev], send_shift.at[k], recv_shift.at[src_dev], dst)

    def step_copy(dst, src_dev, k):
        return remote(step_all.at[me], step_all.at[src_dev], send_step.at[k], recv_step.at[src_dev], dst)

    def noise_copy(dst, src_dev, k):
        row, cols = chunk(dst)
        return remote(noise_hbm.at[:, row, :, cols], noise_all.at[src_dev], send_noise.at[k], recv_noise.at[src_dev], dst)

    def out_copy(dst, src_dev, k):
        row, cols = chunk(src_dev)
        return remote(x_all.at[dst], out_hbm.at[:, row, :, cols], send_out.at[k], recv_out.at[src_dev], dst)

    barrier = pltpu.get_barrier_semaphore()

    for k in sorted(range(1, n), key=lambda k: -min(k, n - k)):
        pl.semaphore_signal(barrier, inc=1, device_id={"time": peer(k)}, device_id_type=pl.DeviceIdType.MESH)

    local = [
        pltpu.make_async_copy(x0_hbm.at[my_row, :, my_cols], x0, local_sem.at[0]),
        pltpu.make_async_copy(noise_hbm.at[:, my_row, :, my_cols], noise_all.at[me], local_sem.at[1]),
    ]
    for copy in local:
        copy.start()
    scale_all[me] = scale[...]
    shift_all[me] = shift[...]
    for t in range(own):
        step_all[me, t:t + 1, :] = jnp.full((1, tok), step[t], F32)

    half = 0.5 * w_in[...].astype(F32)
    top = lax.broadcasted_iota(jnp.int32, (chan, hidden), 0) == 0

    def modulated(scales, shifts):
        scales, shifts = scales.astype(F32), shifts.astype(F32)
        parts = []
        for t in range(own):
            value = half * scales[t:t + 1, :]
            high = value.astype(BF16)
            low = (value - high.astype(F32)).astype(BF16)
            bias = jnp.where(top, 0.5 * shifts[t:t + 1, :], 0.0).astype(BF16)
            parts += [half.astype(BF16), high, low, bias]
        return jnp.transpose(jnp.concatenate(parts, axis=0))

    for copy in local:
        copy.wait()

    xb = x0[...].astype(BF16)
    block = jnp.concatenate([xb, xb, xb, jnp.ones_like(xb)], axis=0)
    nothing = jnp.zeros_like(block)
    both = jnp.concatenate([jnp.concatenate([block, nothing], axis=1), jnp.concatenate([nothing, block], axis=1)], axis=0)

    @pl.loop(0, n)
    def _(q):
        rhs[q] = both

    def put_latents(q, t, xb):
        for j in range(3):
            rhs[q, width * t + chan * j:width * t + chan * (j + 1), tok * t:tok * (t + 1)] = xb

    def first_product(w, q, slot):
        right = rhs[q]
        for part in range(2):
            rows = slice(part * hidden // 2, (part + 1) * hidden // 2)
            hid[slot][rows, :] = jnp.dot(weights[w, rows, :], right, preferred_element_type=F32)

    def activate(slot):
        g = hid[slot][...]
        act[slot][...] = g * (1.0 + jnp.tanh(g * (LIN + CUB * (g * g))))

    def second_product(slot):
        return jnp.dot(w_out[...].astype(F32), act[slot][...], preferred_element_type=F32)

    def sweep(into):
        def finish(q, slot):
            drift = second_product(slot)
            for t in range(own):
                into[q, t] = drift[:, tok * t:tok * (t + 1)] * step_all[q, t:t + 1, :]

        for q in range(2):
            weights[q] = modulated(scale_all[q], shift_all[q])
        first_product(0, 0, 0)

        def trip(i, carry):
            base = i * FIRST_UNROLL
            for u in range(FIRST_UNROLL):
                nxt = lax.rem(base + u + 1, n)
                later = lax.rem(base + u + 2, n)
                weights[later] = modulated(scale_all[later], shift_all[later])
                finish(lax.rem(base + n - 1 + u, n), (u - 1) % SLOTS)
                activate(u % SLOTS)
                first_product(nxt, nxt, (u + 1) % SLOTS)
            return carry

        lax.fori_loop(0, n // FIRST_UNROLL, trip, 0)
        finish(n - 1, (FIRST_UNROLL - 1) % SLOTS)

    pl.semaphore_wait(barrier, n - 1)

    @pl.loop(1, n)
    def _(k):
        far = jnp.where(k % 2 == 1, (n - k + 1) // 2, n - (n - k) // 2)
        scale_copy(peer(far), me, far).start()
        shift_copy(peer(far), me, far).start()
        step_copy(peer(far), me, far).start()

    @pl.loop(1, n)
    def _(k):
        noise_copy(peer(k), me, k).start()

    @pl.loop(1, n)
    def _(k):
        scale_copy(peer(k), source(k), k).wait_recv()
        shift_copy(peer(k), source(k), k).wait_recv()

    @pl.loop(1, n)
    def _(k):
        step_copy(peer(k), source(k), k).wait_recv()

    sweep(drift_mine)

    @pl.loop(1, n)
    def _(k):
        noise_copy(peer(k), source(k), k).wait_recv()

    x = x0[...]
    for q in range(n):
        for t in range(own):
            xb = x.astype(BF16)
            put_latents(q, t, xb)
            if q >= n - 1 - UNROLL and q < n - 1:
                staged[q - (n - 1 - UNROLL), t] = xb
            if q == n - 1 and t == 0:
                run[...] = x
            x = x + (drift_mine[q, t] + noise_all[q, t])

    starts, ends = plan(n, own)

    def pair_of(p):
        q = p + jnp.where(p < 0, n, 0)
        for sweep_end, first in zip(ends[:-1], starts[1:]):
            q = q - jnp.where(p >= sweep_end, n - first, 0)
        return lax.rem(q, n)

    def advance(p, slot, u):
        q = pair_of(p)
        change = second_product(slot)
        opens = p == 0
        for sweep_end in ends[:-1]:
            opens = opens | (p == sweep_end)
        x = jnp.where(opens, x_all[q, 0], run[...])
        for t in range(own):
            x_all[q, t] = x
            if u is not None:
                staged[u, t] = x.astype(BF16)
            x = x + (change[:, tok * t:tok * (t + 1)] * step_all[q, t:t + 1, :] + noise_all[q, t])
        run[...] = x

    x_all[0, 0] = x0[...]
    first_product(0, 0, 0)

    def trip(i, carry):
        base = i * UNROLL
        for u in range(UNROLL):
            late = pair_of(base - 1 - UNROLL + u)
            for t in range(own):
                put_latents(late, t, staged[u, t])
            advance(base - 1 + u, (u - 1) % SLOTS, u)
            activate(u % SLOTS)
            q = pair_of(base + u + 1)
            first_product(q, q, (u + 1) % SLOTS)
        return carry

    trips = ends[-1] // UNROLL
    early = n - UNROLL - 1
    lax.fori_loop(0, trips - 1, trip, 0)

    def deliver(first_dev, count):
        @pl.loop(0, count)
        def _(k):
            dst = first_dev + lax.rem(me + k, count)

            @pl.when(dst != me)
            def _():
                out_copy(dst, me, lax.rem(dst - me + n, n)).start()

    deliver(0, early)
    trip(trips - 1, 0)
    advance(ends[-1] - 1, (UNROLL - 1) % SLOTS, None)
    deliver(early, n - early)

    last = pltpu.make_async_copy(x_all.at[me], out_hbm.at[:, my_row, :, my_cols], local_sem.at[0])
    last.start()

    @pl.loop(1, n)
    def _(k):
        scale_copy(peer(k), me, k).wait_send()
        shift_copy(peer(k), me, k).wait_send()
        step_copy(peer(k), me, k).wait_send()
        noise_copy(peer(k), me, k).wait_send()

    last.wait()

    @pl.loop(1, n)
    def _(k):
        out_copy(peer(k), source(k), k).wait_recv()

    @pl.loop(1, n)
    def _(k):
        out_copy(peer(k), me, k).wait_send()


def solution(mesh):
    n = mesh.shape["time"]

    def body(x_init, w_in, w_out, mod_scale, mod_shift, step_size, noise_inc):
        own, batch, tokens, chan = noise_inc.shape
        hidden = w_in.shape[1]
        tok = batch * tokens // n
        vmem, hbm, smem = (pl.BlockSpec(memory_space=m) for m in (pltpu.VMEM, pl.ANY, pltpu.SMEM))
        out = pl.pallas_call(
            functools.partial(kernel, n, own),
            out_shape=jax.ShapeDtypeStruct((own, batch, chan, tokens), F32),
            in_specs=[hbm, vmem, vmem, vmem, vmem, smem, hbm],
            out_specs=hbm,
            scratch_shapes=[
                pltpu.VMEM((n, hidden, 128), BF16),
                pltpu.VMEM((n, 128, own * tok), BF16),
                pltpu.VMEM((n, own, hidden), BF16),
                pltpu.VMEM((n, own, hidden), BF16),
                pltpu.VMEM((n, own, tok), F32),
            ]
            + [pltpu.VMEM((n, own, chan, tok), F32)] * 3
            + [
                pltpu.VMEM((chan, tok), F32),
                pltpu.VMEM((chan, tok), F32),
                pltpu.VMEM((UNROLL, own, chan, tok), BF16),
            ]
            + [pltpu.VMEM((hidden, own * tok), F32)] * (2 * SLOTS)
            + [pltpu.SemaphoreType.DMA((n,))] * 10
            + [pltpu.SemaphoreType.DMA((2,))],
            compiler_params=pltpu.CompilerParams(collective_id=0, has_side_effects=True, vmem_limit_bytes=40 * 1024 * 1024),
            name="picard",
        )(jnp.swapaxes(x_init, 1, 2), w_in, w_out.T, mod_scale, mod_shift, step_size, jnp.swapaxes(noise_inc, 2, 3))
        return jnp.swapaxes(out, 2, 3)

    return jax.shard_map(
        body,
        mesh=mesh,
        in_specs=(P("data"), P(), P(), P("time"), P("time"), P("time"), P("time", "data")),
        out_specs=P("time", "data"),
        check_vma=False,
    )
```
